32 devices in a mesh: seq: 8 (over y, x, core), head: 4 (over z).
Axes of the slice: x: 2, y: 2, z: 4, core: 2. Of those that a mesh axis runs over, the one named last changes fastest.
Arguments:
- latent: bfloat16 [8, 1024, 2048], P('seq', None, 'head'), may hold values from -6 to 6
- modulation: float32 [9, 2048], replicated, may hold values from -3 to 3
- spatial_qkv: bfloat16 [3, 2048, 2048], P(None, None, 'head')
- spatial_out: bfloat16 [2048, 2048], P('head'), may hold values from -0.125 to 0.125
- temporal_qkv: bfloat16 [3, 2048, 2048], P(None, None, 'head')
- temporal_out: bfloat16 [2048, 2048], P('head'), may hold values from -0.125 to 0.125
- hidden_weight: bfloat16 [2048, 8192], P(None, 'head'), may hold values from -0.125 to 0.125
- output_weight: bfloat16 [8192, 2048], P('head'), may hold values from -0.0625 to 0.0625
Outputs:
- block_out: bfloat16 [8, 1024, 2048], P(None, 'seq', 'head')
The draws below stay inside these ranges and needn't reach their ends.
All inputs are finite; a program needn't handle non-finite values.
Results may differ from the reference program's by a relative error of at most 0.009.
Values may be sent and summed in bfloat16 or wider, within the bound.
A program may use at most 128 MiB of HBM per device.

```python
import jax
import jax.numpy as jnp
from jax import lax

D = 2048
HEADS = 32
FF = 8192
P_SIZE = 1024
HD = 64
FRAMES = 8


def projection_draw(key, salt):
    key = jax.random.fold_in(key, salt)
    first, second, third = jax.random.split(key, 3)
    spread = D ** (-0.5)
    query = jax.random.normal(first, (D, D), jnp.float32) * spread
    keys = jax.random.normal(second, (D, D), jnp.float32) * spread
    values = jax.random.normal(third, (D, D), jnp.float32) * spread
    return jnp.stack([query, keys, values]).astype(jnp.bfloat16)


def draw_spatial_qkv(key, part):
    return projection_draw(key, 11)


def draw_temporal_qkv(key, part):
    return projection_draw(key, 23)


def level_of(rng, extent, cuts, least, high):
    factor_of = 1.0
    for dim, parts in cuts:
        draws = jax.random.uniform(jax.random.fold_in(jax.random.fold_in(rng, 6), dim), (parts,), jnp.float32, least / len(cuts), high / len(cuts))
        factor_of = factor_of * jnp.repeat(jnp.exp(draws), extent[dim] // parts).reshape((-1,) + (1,) * (len(extent) - 1 - dim))
    return factor_of


def normal_values(stream_key, shape, scale, most, cuts=(), kind=jnp.bfloat16):
    drawn = jax.random.normal(stream_key, shape, jnp.float32) * scale
    if len(cuts) > 0:
        drawn = level_of(stream_key, shape, cuts, -0.22, 0.18) * drawn
    return jnp.clip(drawn, min=-most, max=most).astype(kind)


def setup_inputs(seed: int = 0) -> dict:
    arg_keys = jax.random.split(jax.random.key(seed), 9)
    return {
        "latent": normal_values(arg_keys[0], (FRAMES, P_SIZE, D), 1.0, 6.0, ((0, 8), (2, 4))),
        "modulation": normal_values(arg_keys[1], (9, D), 0.5, 3.0, (), jnp.float32),
        "spatial_qkv": draw_spatial_qkv(jax.random.fold_in(arg_keys[8], 71), 0),
        "spatial_out": normal_values(arg_keys[3], (D, D), D ** -0.5, 0.125, ((0, 4),)),
        "temporal_qkv": draw_temporal_qkv(jax.random.fold_in(arg_keys[8], 71), 0),
        "temporal_out": normal_values(arg_keys[5], (D, D), D ** -0.5, 0.125, ((0, 4),)),
        "hidden_weight": normal_values(arg_keys[6], (D, FF), D ** -0.5, 0.125, ((1, 4),)),
        "output_weight": normal_values(arg_keys[7], (FF, D), FF ** -0.5, 0.0625, ((0, 4),)),
    }


def layer_norm(values):
    average = lax.optimization_barrier(jnp.mean(values, axis=-1, keepdims=True))
    centred = values - average
    variance = lax.optimization_barrier(jnp.mean(centred * centred, axis=-1, keepdims=True))
    return centred * lax.rsqrt(variance + 1e-06)

def modulate(stream, modulation, offset):
    normed = layer_norm(stream.astype(jnp.float32))
    return (normed * (1.0 + modulation[offset + 1]) + modulation[offset]).astype(jnp.bfloat16)

def attend(query, keys, values):
    scores = jnp.einsum('glhd,gmhd->ghlm', query.astype(jnp.float32), keys.astype(jnp.float32)) * HD ** (-0.5)
    attn_weights = jax.nn.softmax(scores, axis=-1).astype(jnp.bfloat16)
    return jnp.einsum('ghlm,gmhd->glhd', attn_weights.astype(jnp.float32), values.astype(jnp.float32)).astype(jnp.bfloat16)

def project_three(normed, weights):
    return [jnp.dot(normed, weights[member], preferred_element_type=jnp.float32).astype(jnp.bfloat16) for member in range(3)]

def reference(latent, modulation, spatial_qkv, spatial_out, temporal_qkv, temporal_out, hidden_weight, output_weight):
    frames = latent.shape[0]
    patches = latent.shape[1]

    def split_heads(tensor):
        return tensor.reshape(frames, patches, HEADS, HD)
    normed = modulate(latent, modulation, 0)
    query, keys, values = [split_heads(member) for member in project_three(normed, spatial_qkv)]
    spatial = lax.map(lambda triple: attend(triple[0][None], triple[1][None], triple[2][None])[0], (query, keys, values))
    spatial = spatial.reshape(frames, patches, D)
    branch = jnp.dot(spatial, spatial_out, preferred_element_type=jnp.float32)
    stream_one = (latent.astype(jnp.float32) + modulation[2] * branch).astype(jnp.bfloat16)
    normed = modulate(stream_one, modulation, 3)
    query, keys, values = [jnp.transpose(split_heads(member), (1, 0, 2, 3)) for member in project_three(normed, temporal_qkv)]
    temporal = jnp.transpose(attend(query, keys, values), (1, 0, 2, 3)).reshape(frames, patches, D)
    branch = jnp.dot(temporal, temporal_out, preferred_element_type=jnp.float32)
    stream_two = (stream_one.astype(jnp.float32) + modulation[5] * branch).astype(jnp.bfloat16)
    normed = modulate(stream_two, modulation, 6)
    hidden = jax.nn.gelu(jnp.dot(normed, hidden_weight, preferred_element_type=jnp.float32), approximate=True).astype(jnp.bfloat16)
    branch = jnp.dot(hidden, output_weight, preferred_element_type=jnp.float32)
    return (stream_two.astype(jnp.float32) + modulation[8] * branch).astype(jnp.bfloat16)
```

```python
import functools
import math

import jax
import jax.numpy as jnp
from jax import lax
from jax.experimental import pallas as pl
from jax.experimental.pallas import tpu as pltpu
from jax.sharding import PartitionSpec as P

HD = 64
PAIR = 128
CHUNKS = 2
EXP2_SCALE = HD ** (-0.5) * math.log2(math.e)
BF16 = jnp.bfloat16
NT = (((1,), (1,)), ((), ()))


def layer_norm(values):
    average = jnp.mean(values, axis=-1, keepdims=True)
    centred = values - average
    variance = jnp.mean(centred * centred, axis=-1, keepdims=True)
    return centred * lax.rsqrt(variance + 1e-06)


def modulate(stream, modulation, offset):
    normed = layer_norm(stream.astype(jnp.float32))
    return (normed * (1.0 + modulation[offset + 1]) + modulation[offset]).astype(BF16)


def weighted_values(scores, values):
    top = jnp.max(scores, axis=-1, keepdims=True)
    weights = jnp.exp2((scores - top) * EXP2_SCALE).astype(BF16)
    extended = jnp.concatenate([values, jnp.ones_like(values)], axis=1)
    summed = jnp.dot(weights, extended, preferred_element_type=jnp.float32)
    return summed[:, :HD] / summed[:, HD:]


def spatial_kernel(q_ref, k_ref, v_ref, o_ref):
    outs = []
    for head in range(PAIR // HD):
        lanes = slice(head * HD, (head + 1) * HD)
        scores = lax.dot_general(
            q_ref[0, :, lanes], k_ref[0, :, lanes], NT, preferred_element_type=jnp.float32
        )
        outs.append(weighted_values(scores, v_ref[0, :, lanes]))
    o_ref[0] = jnp.concatenate(outs, axis=1).astype(BF16)


def spatial_attention(query, keys, values):
    frames, patches, width = query.shape
    rows = min(patches, 512)
    return pl.pallas_call(
        spatial_kernel,
        grid=(frames, width // PAIR, patches // rows),
        in_specs=[
            pl.BlockSpec((1, rows, PAIR), lambda f, h, r: (f, r, h)),
            pl.BlockSpec((1, patches, PAIR), lambda f, h, r: (f, 0, h)),
            pl.BlockSpec((1, patches, PAIR), lambda f, h, r: (f, 0, h)),
        ],
        out_specs=pl.BlockSpec((1, rows, PAIR), lambda f, h, r: (f, r, h)),
        out_shape=jax.ShapeDtypeStruct(query.shape, BF16),
        cost_estimate=pl.CostEstimate(
            flops=16 * frames * patches * patches * width,
            bytes_accessed=8 * query.size,
            transcendentals=frames * patches * patches * (width // HD),
        ),
        name="spatial_attention",
    )(query, keys, values)


def temporal_kernel(q_ref, k_ref, v_ref, o_ref):
    frames, group, width = q_ref.shape
    rows = frames * group
    query = q_ref[...].reshape(rows, width)
    keys = k_ref[...].reshape(rows, width)
    values = v_ref[...].reshape(rows, width)
    first = lax.broadcasted_iota(jnp.int32, (rows, rows), 0)
    second = lax.broadcasted_iota(jnp.int32, (rows, rows), 1)
    same_patch = lax.rem(first, group) == lax.rem(second, group)
    outs = []
    for head in range(width // HD):
        lanes = slice(head * HD, (head + 1) * HD)
        scores = lax.dot_general(
            query[:, lanes], keys[:, lanes], NT, preferred_element_type=jnp.float32
        )
        outs.append(
            weighted_values(jnp.where(same_patch, scores, -jnp.inf), values[:, lanes])
        )
    o_ref[...] = jnp.concatenate(outs, axis=1).astype(BF16).reshape(frames, group, width)


def temporal_attention(query, keys, values):
    frames, patches, width = query.shape
    group = min(16, patches)
    spec = pl.BlockSpec((frames, group, width), lambda g: (0, g, 0))
    return pl.pallas_call(
        temporal_kernel,
        grid=(patches // group,),
        in_specs=[spec] * 3,
        out_specs=spec,
        out_shape=jax.ShapeDtypeStruct(query.shape, BF16),
        cost_estimate=pl.CostEstimate(
            flops=16 * frames * frames * patches * group * width,
            bytes_accessed=8 * query.size,
            transcendentals=frames * frames * patches * group * (width // HD),
        ),
        name="temporal_attention",
    )(query, keys, values)


def project_three(normed, weights):
    return [
        jnp.dot(normed, weights[member], preferred_element_type=jnp.float32).astype(BF16)
        for member in range(3)
    ]


def summed_columns(portion, row_block):
    partial = jnp.dot(portion, row_block, preferred_element_type=jnp.float32).astype(BF16)
    return lax.psum_scatter(partial, "head", scatter_dimension=2, tiled=True)


def add_branch(stream, gate, reduced):
    return (stream.astype(jnp.float32) + gate * reduced.astype(jnp.float32)).astype(BF16)


def per_device(
    latent,
    modulation,
    spatial_qkv,
    spatial_out,
    temporal_qkv,
    temporal_out,
    hidden_weight,
    output_weight,
):
    frames_local, patches, width_local = latent.shape
    seq = lax.axis_size("seq")
    patches_local = patches // seq
    piece = patches_local // CHUNKS
    anchor = lax.axis_index("head") * width_local
    local_rows = lax.dynamic_slice_in_dim(modulation, anchor, width_local, 1)
    full_spatial = lax.all_gather(latent, "head", axis=2, tiled=True)
    normed = modulate(full_spatial, modulation, 0)
    query, keys, values = project_three(normed, spatial_qkv)
    spatial = spatial_attention(query, keys, values)

    def chunk_of(tensor, index):
        parts = tensor.reshape(frames_local, seq, CHUNKS, piece, width_local)
        return parts[:, :, index].reshape(frames_local, seq * piece, width_local)

    outs = []
    ones = []
    for index in range(CHUNKS):
        reduced = summed_columns(chunk_of(spatial, index), spatial_out)
        ones.append(add_branch(chunk_of(latent, index), local_rows[2], reduced))
    ones = [
        lax.all_to_all(one, "seq", split_axis=1, concat_axis=0, tiled=True) for one in ones
    ]
    twos = []
    for one in ones:
        full = lax.all_gather(one, "head", axis=2, tiled=True)
        normed = modulate(full, modulation, 3)
        temporal = temporal_attention(*project_three(normed, temporal_qkv))
        reduced = summed_columns(temporal, temporal_out)
        twos.append(add_branch(one, local_rows[5], reduced))
    for two in twos:
        full = lax.all_gather(two, "head", axis=2, tiled=True)
        normed = modulate(full, modulation, 6)
        pre_act = jnp.dot(normed, hidden_weight, preferred_element_type=jnp.float32)
        hidden = jax.nn.gelu(pre_act, approximate=True).astype(BF16)
        reduced = summed_columns(hidden, output_weight)
        outs.append(add_branch(two, local_rows[8], reduced))
    return jnp.concatenate(outs, axis=1)


def solution(mesh):
    in_specs = (
        P("seq", None, "head"),
        P(),
        P(None, None, "head"),
        P("head", None),
        P(None, None, "head"),
        P("head", None),
        P(None, "head"),
        P("head", None),
    )
    out_specs = P(None, "seq", "head")
    return jax.shard_map(
        per_device, mesh=mesh, in_specs=in_specs, out_specs=out_specs, check_vma=False
    )
```
